32 devices in a mesh: member: 8 (over z, x), mp: 4 (over y, core).
Axes of the slice: x: 2, y: 2, z: 4, core: 2. Of those that a mesh axis runs over, the one named last changes fastest.
Arguments:
- latents: bfloat16 [32, 1024, 1024], P('member', 'mp'), may hold values from -6 to 6
- w_first: bfloat16 [1024, 2048], P(None, 'mp'), may hold values from -0.1875 to 0.1875
- w_second: bfloat16 [2048, 1024], P('mp'), may hold values from -0.125 to 0.125
- readout_matrix: bfloat16 [1024, 768], P(None, 'mp'), may hold values from -0.1875 to 0.1875
- observed: float32 [1024, 768], P(('mp', 'member')), may hold values from -9 to 9
- obs_index: int32 [1024], P(('mp', 'member')), may hold values from 0 to 1023, as said below
- valid_mask: int32 [1024], P(('mp', 'member')), may hold values from 0 to 1
Outputs:
- grad_first: float32 [1024, 2048], P(('member', 'mp'))
- grad_second: float32 [2048, 1024], P(('member', 'mp'))
- grad_head: float32 [1024, 768], P(('member', 'mp'))
- loss: float32 [], replicated
The draws below stay inside these ranges and needn't reach their ends.
Inputs may be any that keep to these rules, and one draw needn't show every extreme that they name: obs_index[p] names a record of the same aligned block of 32 patches as p.
All inputs are finite; a program needn't handle non-finite values.
Results may differ from the reference program's by a relative error of at most 0.006.
Values may be sent and summed in bfloat16 or wider, within the bound.
A program may use at most 128 MiB of HBM per device.

```python
import jax
import jax.numpy as jnp
from jax import lax

D = 1024
HID = 2048
OUT = 768
MEMBERS = 32
PATCHES = 1024
P_OWN = 32


def draw_obs_index(key, part):
    subkey = jax.random.fold_in(key, 11)
    base_rows = jnp.arange(PATCHES, dtype=jnp.int32) // P_OWN * P_OWN
    return base_rows + jax.random.randint(subkey, (PATCHES,), 0, P_OWN, dtype=jnp.int32)


def draw_valid_mask(key, part):
    subkey = jax.random.fold_in(key, 23)
    levels = jax.random.randint(subkey, (PATCHES,), 0, 4 * PATCHES, dtype=jnp.int32)
    bounds = PATCHES + 2 * jnp.arange(PATCHES, dtype=jnp.int32)
    return (levels < bounds).astype(jnp.int32)


def block_scale(stream_key, dims, pieces, smallest, largest):
    loudness = 1.0
    for position, parts in pieces:
        steps = jax.random.uniform(jax.random.fold_in(jax.random.fold_in(stream_key, 6), position), (parts,), jnp.float32, smallest / len(pieces), largest / len(pieces))
        loudness = loudness * jnp.repeat(jnp.exp(steps), dims[position] // parts).reshape((-1,) + (1,) * (len(dims) - 1 - position))
    return loudness


def noise(rng, dims, deviation, limit, cuts=(), kind=jnp.bfloat16):
    array = jax.random.normal(rng, dims, jnp.float32) * deviation
    if len(cuts) > 0:
        array = block_scale(rng, dims, cuts, -0.22, 0.18) * array
    return jnp.clip(array, min=-limit, max=limit).astype(kind)


def setup_inputs(seed: int = 0) -> dict:
    key_of = jax.random.split(jax.random.key(seed), 8)
    return {
        "latents": noise(key_of[0], (MEMBERS, PATCHES, D), 1.0, 6.0, ((0, 8), (1, 4))),
        "w_first": noise(key_of[1], (D, HID), D ** -0.5, 0.1875, ((1, 4),)),
        "w_second": noise(key_of[2], (HID, D), HID ** -0.5, 0.125, ((0, 4),)),
        "readout_matrix": noise(key_of[3], (D, OUT), D ** -0.5, 0.1875, ((1, 4),)),
        "observed": noise(key_of[4], (PATCHES, OUT), 1.5, 9.0, ((0, 32),), jnp.float32),
        "obs_index": draw_obs_index(jax.random.fold_in(key_of[7], 71), 0),
        "valid_mask": draw_valid_mask(jax.random.fold_in(key_of[7], 71), 0),
    }


SMOOTHING = 1.0
LOSS_SCALE = 4096.0

def gelu_fn(values):
    return jax.nn.gelu(values, approximate=True)

def gelu_back(preact, upstream):
    return jax.vjp(gelu_fn, preact)[1](upstream)[0]

def row_outer(left_rows, right_rows):
    return lax.dot_general(left_rows, right_rows, (((0,), (0,)), ((), ())), preferred_element_type=jnp.float32)

def reference(latents, w_first, w_second, readout_matrix, observed, obs_index, valid_mask):
    sample_indices = latents.shape[0]
    token_rows = latents.reshape(-1, latents.shape[2])
    preact = jnp.dot(token_rows, w_first, preferred_element_type=jnp.float32)
    hidden = gelu_fn(preact).astype(jnp.bfloat16)
    skip_activation = (token_rows.astype(jnp.float32) + jnp.dot(hidden, w_second, preferred_element_type=jnp.float32)).astype(jnp.bfloat16)
    prediction_lines = jnp.dot(skip_activation, readout_matrix, preferred_element_type=jnp.float32).astype(jnp.bfloat16)
    predicted_samples = prediction_lines.reshape(sample_indices, -1, readout_matrix.shape[1]).astype(jnp.float32)
    target = observed[obs_index.astype(jnp.int32)]
    gram_matrix = jnp.einsum('mpo,npo->pmn', predicted_samples, predicted_samples, precision=lax.Precision.HIGHEST)
    squares = lax.optimization_barrier(jnp.sum(predicted_samples * predicted_samples, axis=2)).T
    dist_sq = squares[:, :, None] + squares[:, None, :] - 2.0 * gram_matrix
    spread = jnp.sqrt(dist_sq + SMOOTHING)
    kernel = 1.0 / spread
    kernel_sum = lax.optimization_barrier(jnp.sum(kernel, axis=2))
    pulled = jnp.einsum('pmn,npo->mpo', kernel, predicted_samples, precision=lax.Precision.HIGHEST)
    offset = predicted_samples - target[None]
    error_norm = jnp.sqrt(lax.optimization_barrier(jnp.sum(offset * offset, axis=2)) + SMOOTHING)
    repulse = predicted_samples * kernel_sum.T[:, :, None] - pulled
    validity = valid_mask.astype(jnp.float32)
    grad_raw = (LOSS_SCALE * validity[None, :, None] * (offset / (sample_indices * error_norm[:, :, None]) - repulse / (sample_indices * sample_indices))).astype(jnp.bfloat16)
    scores = validity * (lax.optimization_barrier(jnp.mean(error_norm, axis=0)) - lax.optimization_barrier(jnp.sum(spread, axis=(1, 2))) / (2.0 * sample_indices * sample_indices))
    valid_total = jnp.maximum(jnp.sum(validity), 1.0)
    loss = jnp.sum(scores) / valid_total
    grad_rows = grad_raw.reshape(-1, readout_matrix.shape[1])
    resid_grad = jnp.dot(grad_rows, readout_matrix.T, preferred_element_type=jnp.float32).astype(jnp.bfloat16)
    hidden_grad = jnp.dot(resid_grad, w_second.T, preferred_element_type=jnp.float32)
    preact_grad = gelu_back(preact, hidden_grad).astype(jnp.bfloat16)
    grad_scale = 1.0 / valid_total
    return (row_outer(token_rows, preact_grad) * grad_scale, row_outer(hidden, resid_grad) * grad_scale, row_outer(skip_activation, grad_rows) * grad_scale, loss)
```

```python
import jax
import jax.numpy as jnp
from jax import lax
from jax.sharding import PartitionSpec as P

SMOOTHING = 1.0
LOSS_SCALE = 4096.0


def gelu_fn(values):
    return jax.nn.gelu(values, approximate=True)


def gelu_back(preact, upstream):
    return jax.vjp(gelu_fn, preact)[1](upstream)[0]


def row_outer(left_rows, right_rows):
    return lax.dot_general(
        left_rows, right_rows, (((0,), (0,)), ((), ())), preferred_element_type=jnp.float32
    )


def bit_count(axis):
    return lax.axis_size(axis).bit_length() - 1


def swap(array, axis, bit):
    size = lax.axis_size(axis)
    return lax.ppermute(array, axis, [(i, i ^ (1 << bit)) for i in range(size)])


def my_bit(axis, bit):
    return (lax.axis_index(axis) >> bit) & 1


def gather_blocks(block, axis, dim):
    bits = bit_count(axis)
    pieces = {0: block}
    for bit in reversed(range(bits)):
        for relative in list(pieces):
            pieces[relative ^ (1 << bit)] = swap(pieces[relative], axis, bit)
    ordered = []
    for wanted in range(1 << bits):
        left = [pieces[relative] for relative in range(1 << bits)]
        for bit in range(bits):
            want = (wanted >> bit) & 1
            flipped = my_bit(axis, bit) == 1
            left = [
                jnp.where(flipped, left[2 * i + 1 - want], left[2 * i + want])
                for i in range(len(left) // 2)
            ]
        ordered.append(left[0])
    return jnp.concatenate(ordered, axis=dim)


def scatter_sum(total, order):
    across, within = bit_count("member"), bit_count("mp")
    remaining = [("member", b) for b in reversed(range(across))]
    remaining += [("mp", b) for b in reversed(range(within))]
    rows, columns = total.shape
    share = rows >> len(remaining)
    for stage in order:
        place = remaining.index(stage)
        remaining = remaining[:place] + remaining[place + 1 :]
        halves = total.reshape(1 << place, 2, -1, columns)
        mine = my_bit(*stage)
        sent = lax.dynamic_index_in_dim(halves, 1 - mine, 1, keepdims=False)
        kept = lax.dynamic_index_in_dim(halves, mine, 1, keepdims=False)
        got = swap(sent.astype(jnp.bfloat16), *stage)
        total = kept.astype(jnp.float32) + got.astype(jnp.float32)
        total = total.reshape(-1, columns)
    return total.reshape(share, columns)


def everywhere_sum(values):
    for axis in ("mp", "member"):
        for bit in range(bit_count(axis)):
            values = values + swap(values, axis, bit)
    return values


def stage_orders():
    across, within = bit_count("member"), bit_count("mp")
    first = [("mp", 0)]
    rest = [("member", b) for b in range(1, across)]
    mp_rest = [("mp", b) for b in range(1, within)]
    low = [("member", 0)]
    return (
        first + mp_rest + low + rest[::-1],
        first + low + mp_rest + rest[::-1],
    )


def per_device(latents, w_first, w_second, readout_matrix, observed, obs_index, valid_mask):
    feature_width = latents.shape[2]
    full_first = gather_blocks(w_first, "mp", 1)
    full_second = gather_blocks(w_second, "mp", 0)
    complete_head = gather_blocks(readout_matrix, "mp", 1)
    regrouped = lax.all_to_all(latents, "member", split_axis=1, concat_axis=0, tiled=True)
    sample_indices, owned_count, _ = regrouped.shape
    token_rows = regrouped.reshape(sample_indices * owned_count, feature_width)
    preact = jnp.dot(token_rows, full_first, preferred_element_type=jnp.float32)
    hidden = gelu_fn(preact).astype(jnp.bfloat16)
    skip_activation = (
        token_rows.astype(jnp.float32)
        + jnp.dot(hidden, full_second, preferred_element_type=jnp.float32)
    ).astype(jnp.bfloat16)
    prediction_lines = jnp.dot(
        skip_activation, complete_head, preferred_element_type=jnp.float32
    ).astype(jnp.bfloat16)
    prediction_lines = lax.optimization_barrier(prediction_lines)
    ensemble = prediction_lines.reshape(sample_indices, owned_count, -1)
    offset_row = (
        lax.axis_index("mp") * lax.axis_size("member") + lax.axis_index("member")
    ) * owned_count
    target = jnp.take(observed, obs_index - offset_row, axis=0)
    predicted_samples = ensemble.astype(jnp.float32)
    gram_matrix = jnp.einsum(
        "mpo,npo->pmn", ensemble, ensemble, preferred_element_type=jnp.float32
    )
    squares = jnp.sum(predicted_samples * predicted_samples, axis=2).T
    dist_sq = squares[:, :, None] + squares[:, None, :] - 2.0 * gram_matrix
    spread = jnp.sqrt(dist_sq + SMOOTHING)
    kernel = 1.0 / spread
    kernel_sum = jnp.sum(kernel, axis=2)
    pulled = jnp.einsum("pmn,npo->mpo", kernel, predicted_samples, precision=lax.Precision.HIGHEST)
    offset = predicted_samples - target[None]
    error_norm = jnp.sqrt(jnp.sum(offset * offset, axis=2) + SMOOTHING)
    repulse = predicted_samples * kernel_sum.T[:, :, None] - pulled
    validity = valid_mask.astype(jnp.float32)
    grad_raw = (
        LOSS_SCALE
        * validity[None, :, None]
        * (
            offset / (sample_indices * error_norm[:, :, None])
            - repulse / (sample_indices * sample_indices)
        )
    ).astype(jnp.bfloat16)
    scores = validity * (
        jnp.mean(error_norm, axis=0)
        - jnp.sum(spread, axis=(1, 2)) / (2.0 * sample_indices * sample_indices)
    )
    totals = everywhere_sum(
        jnp.stack([jnp.full((128,), jnp.sum(scores)), jnp.full((128,), jnp.sum(validity))])
    )
    valid_total = jnp.maximum(totals[1, 0], 1.0)
    grad_scale = 1.0 / valid_total
    grad_rows = grad_raw.reshape(sample_indices * owned_count, -1)
    order_a, order_b = stage_orders()

    def reduced(left, right):
        half = right.shape[1] // 2
        local = row_outer(left, right).astype(jnp.bfloat16)
        return jnp.concatenate(
            [
                scatter_sum(local[:, :half], order_a) * grad_scale,
                scatter_sum(local[:, half:], order_b) * grad_scale,
            ],
            axis=1,
        )

    sum_head = reduced(skip_activation, grad_rows)
    resid_grad = jnp.dot(grad_rows, complete_head.T, preferred_element_type=jnp.float32).astype(
        jnp.bfloat16
    )
    sum_second = reduced(hidden, resid_grad)
    hidden_grad = jnp.dot(resid_grad, full_second.T, preferred_element_type=jnp.float32)
    preact_grad = gelu_back(preact, hidden_grad).astype(jnp.bfloat16)
    sum_first = reduced(token_rows, preact_grad)
    return sum_first, sum_second, sum_head, totals[0, 0] / valid_total


def solution(mesh):
    return jax.shard_map(
        per_device,
        mesh=mesh,
        in_specs=(
            P("member", "mp", None),
            P(None, "mp"),
            P("mp", None),
            P(None, "mp"),
            P(("mp", "member"), None),
            P(("mp", "member")),
            P(("mp", "member")),
        ),
        out_specs=(
            P(("member", "mp"), None),
            P(("member", "mp"), None),
            P(("member", "mp"), None),
            P(),
        ),
        check_vma=False,
    )
```

```python
import jax
import jax.numpy as jnp
from jax import lax
from jax.sharding import PartitionSpec as P

SMOOTHING = 1.0
LOSS_SCALE = 4096.0


def gelu_fn(values):
    return jax.nn.gelu(values, approximate=True)


def gelu_back(preact, upstream):
    return jax.vjp(gelu_fn, preact)[1](upstream)[0]


def row_outer(left_rows, right_rows):
    return lax.dot_general(
        left_rows, right_rows, (((0,), (0,)), ((), ())), preferred_element_type=jnp.float32
    )


def bit_count(axis):
    return lax.axis_size(axis).bit_length() - 1


def swap(array, axis, bit):
    size = lax.axis_size(axis)
    return lax.ppermute(array, axis, [(i, i ^ (1 << bit)) for i in range(size)])


def my_bit(axis, bit):
    return (lax.axis_index(axis) >> bit) & 1


def gather_blocks(block, axis, dim):
    bits = bit_count(axis)
    pieces = {0: block}
    for bit in reversed(range(bits)):
        for relative in list(pieces):
            pieces[relative ^ (1 << bit)] = swap(pieces[relative], axis, bit)
    ordered = []
    for wanted in range(1 << bits):
        left = [pieces[relative] for relative in range(1 << bits)]
        for bit in range(bits):
            want = (wanted >> bit) & 1
            flipped = my_bit(axis, bit) == 1
            left = [
                jnp.where(flipped, left[2 * i + 1 - want], left[2 * i + want])
                for i in range(len(left) // 2)
            ]
        ordered.append(left[0])
    return jnp.concatenate(ordered, axis=dim), pieces[1 << (bits - 1)]


def all_stages():
    across, within = bit_count("member"), bit_count("mp")
    return [("member", b) for b in reversed(range(across))] + [
        ("mp", b) for b in reversed(range(within))
    ]


def halve(state, stage):
    total, remaining = state
    place = remaining.index(stage)
    columns = total.shape[1]
    halves = total.reshape(1 << place, 2, -1, columns)
    mine = my_bit(*stage)
    sent = lax.dynamic_index_in_dim(halves, 1 - mine, 1, keepdims=False)
    kept = lax.dynamic_index_in_dim(halves, mine, 1, keepdims=False)
    got = swap(sent.astype(jnp.bfloat16), *stage)
    total = kept.astype(jnp.float32) + got.astype(jnp.float32)
    return total.reshape(-1, columns), remaining[:place] + remaining[place + 1 :]


def finish(state, order):
    for stage in order:
        if stage in state[1]:
            state = halve(state, stage)
    return state[0]


def after(value, *others):
    return lax.optimization_barrier((value, *others))


def stage_orders():
    across, within = bit_count("member"), bit_count("mp")
    first = [("mp", 0)]
    rest = [("member", b) for b in range(1, across)]
    mp_rest = [("mp", b) for b in range(1, within)]
    low = [("member", 0)]
    return (
        first + mp_rest + low + rest,
        first + low + mp_rest + rest,
    )


def per_device(latents, w_first, w_second, readout_matrix, observed, obs_index, valid_mask):
    feature_width = latents.shape[2]
    full_first, arrived = gather_blocks(w_first, "mp", 1)
    w_second, _ = after(w_second, arrived)
    full_second, arrived = gather_blocks(w_second, "mp", 0)
    readout_matrix, _, full_first = after(readout_matrix, arrived, full_first)
    complete_head, _ = gather_blocks(readout_matrix, "mp", 1)
    regrouped = lax.all_to_all(latents, "member", split_axis=1, concat_axis=0, tiled=True)
    sample_indices, owned_count, _ = regrouped.shape
    token_rows = regrouped.reshape(sample_indices * owned_count, feature_width)
    preact = jnp.dot(token_rows, full_first, preferred_element_type=jnp.float32)
    hidden = gelu_fn(preact).astype(jnp.bfloat16)
    skip_activation = (
        token_rows.astype(jnp.float32)
        + jnp.dot(hidden, full_second, preferred_element_type=jnp.float32)
    ).astype(jnp.bfloat16)
    prediction_lines = jnp.dot(
        skip_activation, complete_head, preferred_element_type=jnp.float32
    ).astype(jnp.bfloat16)
    prediction_lines = lax.optimization_barrier(prediction_lines)
    ensemble = prediction_lines.reshape(sample_indices, owned_count, -1)
    offset_row = (
        lax.axis_index("mp") * lax.axis_size("member") + lax.axis_index("member")
    ) * owned_count
    target = jnp.take(observed, obs_index - offset_row, axis=0)
    predicted_samples = ensemble.astype(jnp.float32)
    gram_matrix = jnp.einsum(
        "mpo,npo->pmn", ensemble, ensemble, preferred_element_type=jnp.float32
    )
    squares = jnp.sum(predicted_samples * predicted_samples, axis=2).T
    dist_sq = squares[:, :, None] + squares[:, None, :] - 2.0 * gram_matrix
    spread = jnp.sqrt(dist_sq + SMOOTHING)
    kernel = 1.0 / spread
    kernel_sum = jnp.sum(kernel, axis=2)
    pulled = jnp.einsum("pmn,npo->mpo", kernel, predicted_samples, precision=lax.Precision.HIGHEST)
    offset = predicted_samples - target[None]
    error_norm = jnp.sqrt(jnp.sum(offset * offset, axis=2) + SMOOTHING)
    repulse = predicted_samples * kernel_sum.T[:, :, None] - pulled
    validity = valid_mask.astype(jnp.float32)
    grad_raw = (
        LOSS_SCALE
        * validity[None, :, None]
        * (
            offset / (sample_indices * error_norm[:, :, None])
            - repulse / (sample_indices * sample_indices)
        )
    ).astype(jnp.bfloat16)
    scores = validity * (
        jnp.mean(error_norm, axis=0)
        - jnp.sum(spread, axis=(1, 2)) / (2.0 * sample_indices * sample_indices)
    )
    totals = jnp.stack([jnp.full((128,), jnp.sum(scores)), jnp.full((128,), jnp.sum(validity))])
    stages = all_stages()
    waiting = list(stages)
    grad_rows = grad_raw.reshape(sample_indices * owned_count, -1)
    order_a, order_b = stage_orders()

    def local_sum(left, right):
        return row_outer(left, right).astype(jnp.bfloat16)

    def totals_step(values):
        return values + swap(values, *waiting.pop()) if waiting else values

    head = local_sum(skip_activation, grad_rows)
    grad_rows, head = after(grad_rows, head)
    head = halve((head, stages), order_b[0])
    totals = totals_step(totals)
    resid_grad = jnp.dot(grad_rows, complete_head.T, preferred_element_type=jnp.float32).astype(
        jnp.bfloat16
    )
    resid_grad, head_sum, totals = after(resid_grad, head[0], totals)
    head = halve((head_sum, head[1]), order_b[1])
    totals = totals_step(totals)
    second = local_sum(hidden, resid_grad)
    resid_grad, second, head_sum, totals = after(resid_grad, second, head[0], totals)
    head = halve((head_sum, head[1]), order_b[2])
    second = halve((second, stages), order_a[0])
    totals = totals_step(totals)
    hidden_grad = jnp.dot(resid_grad, full_second.T, preferred_element_type=jnp.float32)
    preact_grad = gelu_back(preact, hidden_grad).astype(jnp.bfloat16)
    preact_grad, second_sum, head_sum, totals = after(preact_grad, second[0], head[0], totals)
    second = (second_sum, second[1])
    head = (head_sum, head[1])
    while waiting:
        totals = totals_step(totals)
    valid_total = jnp.maximum(totals[1, 0], 1.0)
    grad_scale = 1.0 / valid_total
    half = preact_grad.shape[1] // 2
    first_a = local_sum(token_rows, preact_grad[:, :half])
    first_b = local_sum(token_rows, preact_grad[:, half:])
    sum_head = finish(head, order_b)
    sum_second = finish(second, order_a)
    sum_first = jnp.concatenate(
        [finish((first_a, stages), order_b), finish((first_b, stages), order_a)], axis=1
    )
    return (
        sum_first * grad_scale,
        sum_second * grad_scale,
        sum_head * grad_scale,
        totals[0, 0] / valid_total,
    )


def solution(mesh):
    return jax.shard_map(
        per_device,
        mesh=mesh,
        in_specs=(
            P("member", "mp", None),
            P(None, "mp"),
            P("mp", None),
            P(None, "mp"),
            P(("mp", "member"), None),
            P(("mp", "member")),
            P(("mp", "member")),
        ),
        out_specs=(
            P(("member", "mp"), None),
            P(("member", "mp"), None),
            P(("member", "mp"), None),
            P(),
        ),
        check_vma=False,
    )
```
